32 devices in a mesh: seq: 32 (over z, y, x, core), head: 1.
Axes of the slice: x: 2, y: 2, z: 4, core: 2. Of those that a mesh axis runs over, the one named last changes fastest.
Arguments:
- hidden: bfloat16 [4096, 1024], P('seq'), may hold values from -6 to 6
- query_weight: bfloat16 [1024, 512], P(None, 'head'), may hold values from -0.1875 to 0.1875
- key_weight: bfloat16 [1024, 512], P(None, 'head'), may hold values from -0.1875 to 0.1875
- values: bfloat16 [4096, 512], P('seq', 'head'), may hold values from -6 to 6
- grad_out: bfloat16 [4096, 512], P('seq', 'head'), may hold values from -6 to 6
- random_feats: float32 [8, 64, 256], P('head'), may hold values from -4 to 4
Outputs:
- grad_hidden: float32 [4096, 1024], P('seq')
- grad_values: bfloat16 [4096, 512], P('seq', 'head')
- grad_query_weight: float32 [1024, 512], P('seq', 'head')
- grad_key_weight: float32 [1024, 512], P('seq', 'head')
The draws below stay inside these ranges and needn't reach their ends.
All inputs are finite; a program needn't handle non-finite values.
Results may differ from the reference program's by a relative error of at most 0.0038.
Values sent between devices are 32-bit elements; how exact they have to be, the bound alone decides.
A program may use at most 64 MiB of HBM per device.

```python
import jax
import jax.numpy as jnp
from jax import lax

D = 1024
HEADS = 8
DH = 64
M = 256
E = 512
S = 4096


def raised(drawn, own_key, source, target, blocks, factor):
    owner, partner = [(jnp.arange(drawn.shape[dim]) // (drawn.shape[dim] // blocks)).reshape([-1 if axis == dim else 1 for axis in range(drawn.ndim)]) for dim in (source, target)]
    chosen = jax.random.permutation(own_key, blocks)[partner]
    strong = (owner == chosen) | (owner == (partner + blocks // 2) % blocks)
    return jnp.where(strong, factor * drawn, drawn)


def steps_of(key, dims, split, least, top_value):
    def one(position, blocks):
        steps = jax.random.uniform(jax.random.fold_in(jax.random.fold_in(key, 6), position), (blocks,), jnp.float32, least / len(split), top_value / len(split))
        return jnp.repeat(jnp.exp(steps), dims[position] // blocks).reshape((-1,) + (1,) * (len(dims) - position - 1))

    gain = one(*split[0])
    for cut in split[1:]:
        gain = gain * one(*cut)
    return gain


def normal_values(own_key, extent, spread, reach, cuts=(), kind=jnp.bfloat16):
    result = jax.random.normal(own_key, extent, jnp.float32) * spread
    if len(cuts) > 0:
        result = steps_of(own_key, extent, cuts, -0.22, 0.18) * result
    return jnp.clip(result, min=-reach, max=reach).astype(kind)


def noise_with(key, dims, deviation, limit, split, heavy, dtype=jnp.bfloat16):
    entries = deviation * jax.random.normal(key, dims, jnp.float32)
    if split:
        entries = entries * steps_of(key, dims, split, -0.22, 0.18)
    return jnp.clip(raised(entries, jax.random.fold_in(key, 3), *heavy), -limit, limit).astype(dtype)


def setup_inputs(seed: int = 0) -> dict:
    key_of = jax.random.split(jax.random.key(seed), 7)
    return {
        "hidden": noise_with(key_of[0], (S, D), 1.0, 6.0, ((0, 32),), (0, 1, 32, 2.75)),
        "query_weight": normal_values(key_of[1], (D, E), D ** -0.5, 0.1875),
        "key_weight": normal_values(key_of[2], (D, E), D ** -0.5, 0.1875),
        "values": normal_values(key_of[3], (S, E), 1.0, 6.0, ((0, 32),)),
        "grad_out": normal_values(key_of[4], (S, E), 1.0, 6.0, ((0, 32),)),
        "random_feats": normal_values(key_of[5], (HEADS, DH, M), 1.0, 4.0, (), jnp.float32),
    }


HIGH = lax.Precision.HIGHEST

def features(rows, table):
    logits = jnp.dot(rows, table, precision=HIGH)
    half_norm = 0.5 * lax.optimization_barrier(jnp.sum(rows * rows, axis=1, keepdims=True))
    return jnp.exp(logits - half_norm) * M ** (-0.5)

def feature_grad(rows, feats, grads, table, feature_scale):
    weighted = feats * grads
    back = jnp.dot(weighted, table.T, precision=HIGH)
    return (back - rows * lax.optimization_barrier(jnp.sum(weighted, axis=1, keepdims=True))) * feature_scale

def one_head(packed):
    query_rows, key_rows, value_rows, upstream, table = packed
    feature_scale = DH ** (-0.25)
    query_feats = features(query_rows, table)
    key_feats = features(key_rows, table)
    value_state = jnp.dot(value_rows.T, key_feats, precision=HIGH)
    normalizer = lax.optimization_barrier(jnp.sum(key_feats, axis=0))
    numerator = jnp.dot(query_feats, value_state.T, precision=HIGH)
    denominator = jnp.dot(query_feats, normalizer, precision=HIGH)
    attended = numerator / denominator[:, None]
    grad_numer = upstream / denominator[:, None]
    grad_denom = -lax.optimization_barrier(jnp.sum(upstream * attended, axis=1)) / denominator
    grad_qfeat = jnp.dot(grad_numer, value_state, precision=HIGH) + grad_denom[:, None] * normalizer[None, :]
    grad_state = jnp.dot(grad_numer.T, query_feats, precision=HIGH)
    grad_normal = jnp.dot(grad_denom, query_feats, precision=HIGH)
    grad_kfeat = jnp.dot(value_rows, grad_state, precision=HIGH) + grad_normal[None, :]
    grad_value = jnp.dot(key_feats, grad_state.T, precision=HIGH)
    grad_query = feature_grad(query_rows, query_feats, grad_qfeat, table, feature_scale)
    grad_key = feature_grad(key_rows, key_feats, grad_kfeat, table, feature_scale)
    return (grad_query, grad_key, grad_value)

def split_heads(matrix):
    return matrix.reshape(S, HEADS, DH).transpose(1, 0, 2)

def join_heads(stacked):
    return stacked.transpose(1, 0, 2).reshape(S, E)

def reference(hidden, query_weight, key_weight, values, grad_out, random_feats):
    hidden_f = hidden.astype(jnp.float32)
    wq_f = query_weight.astype(jnp.float32)
    wk_f = key_weight.astype(jnp.float32)
    feature_scale = DH ** (-0.25)
    query_all = jnp.dot(hidden_f, wq_f, precision=HIGH) * feature_scale
    key_all = jnp.dot(hidden_f, wk_f, precision=HIGH) * feature_scale
    grad_query, grad_key, grad_value = lax.map(one_head, (split_heads(query_all), split_heads(key_all), split_heads(values.astype(jnp.float32)), split_heads(grad_out.astype(jnp.float32)), random_feats))
    dq_round = join_heads(grad_query).astype(jnp.bfloat16).astype(jnp.float32)
    dk_round = join_heads(grad_key).astype(jnp.bfloat16).astype(jnp.float32)
    grad_values = join_heads(grad_value).astype(jnp.bfloat16)
    grad_query_weight = jnp.dot(hidden_f.T, dq_round, precision=HIGH)
    grad_key_weight = jnp.dot(hidden_f.T, dk_round, precision=HIGH)
    grad_hidden = jnp.dot(dq_round, wq_f.T, precision=HIGH) + jnp.dot(dk_round, wk_f.T, precision=HIGH)
    return (grad_hidden, grad_values, grad_query_weight, grad_key_weight)
```

```python
import functools

import jax
import jax.numpy as jnp
from jax import lax
from jax.experimental import pallas as pl
from jax.experimental.pallas import tpu as pltpu
from jax.sharding import PartitionSpec as P

HIGHEST = lax.Precision.HIGHEST
HIGH = lax.Precision.HIGH
LANES = 128


def phase_orders(count):
    depth = count.bit_length() - 1
    middle = list(range(1, depth - 1))
    return [[0] + middle[s:] + middle[:s] + [depth - 1] for s in range(3)]


class Peers:
    def __init__(self, count):
        self.count = count
        self.depth = count.bit_length() - 1
        self.me = lax.axis_index("seq")
        self.bits = [(self.me // 2**b) % 2 for b in range(self.depth)]
        self.ids = [self.me + (1 - 2 * self.bits[b]) * 2**b for b in range(self.depth)]

    def greet(self):
        barrier = pltpu.get_barrier_semaphore()
        for peer in self.ids:
            pl.semaphore_signal(
                barrier, inc=1, device_id={"seq": peer}, device_id_type=pl.DeviceIdType.MESH
            )
        pl.semaphore_wait(barrier, self.depth)

    def send(self, src, dst, sends, recvs, bit):
        copy = pltpu.make_async_remote_copy(
            src_ref=src,
            dst_ref=dst,
            send_sem=sends,
            recv_sem=recvs,
            device_id={"seq": self.ids[bit]},
            device_id_type=pl.DeviceIdType.MESH,
        )
        copy.start()
        return copy


class Halving:
    def __init__(self, peers, order, buf, recv, sends, recvs):
        self.peers, self.order = peers, order
        self.buf, self.recv, self.sends, self.recvs = buf, recv, sends, recvs
        self.offs = [0]
        for p, bit in enumerate(order):
            self.offs.append(self.offs[-1] + peers.bits[bit] * (peers.count >> (p + 1)))
        self.place = self.offs[-1]

    def start(self, p):
        half = self.peers.count >> (p + 1)
        bit = self.order[p]
        other = self.offs[p] + (1 - self.peers.bits[bit]) * half
        self.landed = self.recv.at[pl.ds(self.peers.count - 2 * half, half)]
        self.copy = self.peers.send(
            self.buf.at[pl.ds(other, half)], self.landed, self.sends.at[p], self.recvs.at[p], bit
        )

    def finish(self, p):
        half = self.peers.count >> (p + 1)
        self.copy.wait()
        kept = pl.ds(self.offs[p + 1], half)
        self.buf[kept] += self.landed[...]


class Doubling:
    def __init__(self, halving, full, sends, recvs):
        self.halving, self.full, self.sends, self.recvs = halving, full, sends, recvs
        self.peers = halving.peers

    def load(self):
        place = pl.ds(self.halving.place, 1)
        self.full[place] = self.halving.buf[place]

    def start(self, p):
        half = self.peers.count >> (p + 1)
        owned = self.full.at[pl.ds(self.halving.offs[p + 1], half)]
        self.copy = self.peers.send(
            owned, owned, self.sends.at[p], self.recvs.at[p], self.halving.order[p]
        )

    def finish(self, p):
        self.copy.wait()


class SmallSum:
    def __init__(self, peers, order, sent, recv, sends, recvs):
        self.peers, self.order = peers, order
        self.sent, self.recv, self.sends, self.recvs = sent, recv, sends, recvs

    def start(self, p):
        self.copy = self.peers.send(
            self.sent.at[p], self.recv.at[p], self.sends.at[p], self.recvs.at[p], self.order[p]
        )

    def finish(self, p):
        self.copy.wait()
        self.sent[p + 1] = self.sent[p] + self.recv[p]


def fill_blocks(halvings, side, rows_ref, grads_ref):
    count = halvings[0].peers.count
    block = halvings[0].buf.shape[1]
    rows = rows_ref.shape[1]
    step = min(rows, max(block, 256))
    for first in range(0, rows, step):
        part = jnp.dot(
            rows_ref[side, pl.ds(first, step), :], grads_ref[...], preferred_element_type=jnp.float32
        )
        for b in range(step // block):
            rest = first // block + b
            for s, h in enumerate(halvings):
                spot = sum(
                    ((rest >> (bit - 1)) & 1) * (count >> (p + 1))
                    for p, bit in enumerate(h.order)
                    if p > 0
                )
                h.buf[side * (count // 2) + spot] = part[
                    b * block : (b + 1) * block, s * LANES : (s + 1) * LANES
                ]


def comm_kernel(count, state_streams, grad_streams, *refs):
    refs = list(refs)
    take = lambda k: [refs.pop(0) for _ in range(k)]
    has_state, has_grad = state_streams > 0, grad_streams > 0
    if has_state:
        state_ref, normal_ref = take(2)
    if has_grad:
        rows_ref, grads_ref = take(2)
    if has_state:
        state_out, normal_out = take(2)
    if has_grad:
        (grad_out,) = take(1)
    if has_state:
        state_bufs, state_recvs, state_full = (take(state_streams) for _ in range(3))
        small_sent, small_recv, small_s, small_r = take(4)
    if has_grad:
        grad_bufs, grad_recvs = (take(grad_streams) for _ in range(2))
    sends, recvs = take(2)

    peers = Peers(count)
    orders = phase_orders(count)
    depth = peers.depth
    sums, small, outs, grads = [], [], [], []
    slot = 0
    if has_state:
        for s in range(state_streams):
            sums.append(
                Halving(peers, orders[s % 3], state_bufs[s], state_recvs[s], sends.at[slot], recvs.at[slot])
            )
            outs.append(Doubling(sums[-1], state_full[s], sends.at[slot + 1], recvs.at[slot + 1]))
            slot += 2
            state_bufs[s][...] = state_ref[:, :, s * LANES : (s + 1) * LANES]
        small.append(SmallSum(peers, orders[0], small_sent, small_recv, small_s, small_r))
        small_sent[0] = normal_ref[...]
    if has_grad:
        for s in range(grad_streams):
            order = orders[(s + state_streams) % 3]
            grads.append(Halving(peers, order, grad_bufs[s], grad_recvs[s], sends.at[slot], recvs.at[slot]))
            slot += 1

    peers.greet()
    for h in sums + small:
        h.start(0)
    if has_grad:
        core = peers.bits[0]
        fill_blocks(grads, 1 - core, rows_ref, grads_ref)
        for h in grads:
            h.start(0)
        fill_blocks(grads, core, rows_ref, grads_ref)

    grad_steps = [(h, p) for p in range(depth) for h in grads]
    for p in range(depth):
        for h in sums + small:
            h.finish(p)
            if p + 1 < depth:
                h.start(p + 1)
            elif h in sums:
                gather = outs[sums.index(h)]
                gather.load()
                gather.start(depth - 1)
        if p % 2 == 1 or not has_state:
            for h in grads:
                step = p // 2 if has_state else p
                h.finish(step)
                if step + 1 < depth:
                    h.start(step + 1)
    done = depth // 2 if has_state else depth
    for p in reversed(range(depth)):
        for h in outs:
            h.finish(p)
            if p > 0:
                h.start(p - 1)
        if p % 2 == 0 and done < depth:
            for h in grads:
                h.finish(done)
                if done + 1 < depth:
                    h.start(done + 1)
            done += 1
    while done < depth:
        for h in grads:
            h.finish(done)
            if done + 1 < depth:
                h.start(done + 1)
        done += 1
    if has_state:
        for s in range(state_streams):
            state_out[:, :, s * LANES : (s + 1) * LANES] = state_full[s][...]
        normal_out[...] = small_sent[depth]
    for s, h in enumerate(grads):
        grad_out[:, s * LANES : (s + 1) * LANES] = h.buf[h.place]


def communicate(count, call, state=None, grad=None):
    depth = count.bit_length() - 1
    args, shapes, scratch = [], [], []
    f32 = jnp.float32
    state_streams = grad_streams = 0
    if state is not None:
        total, normal = state
        groups, head_dim, feats = total.shape
        rows = groups * head_dim // count
        args += [total.reshape(count, rows, feats), normal]
        shapes += [
            jax.ShapeDtypeStruct((count, rows, feats), f32),
            jax.ShapeDtypeStruct(normal.shape, f32),
        ]
        state_streams = feats // LANES
        scratch += [pltpu.VMEM((count, rows, LANES), f32)] * state_streams
        scratch += [pltpu.VMEM((count - 1, rows, LANES), f32)] * state_streams
        scratch += [pltpu.VMEM((count, rows, LANES), f32)] * state_streams
        scratch += [
            pltpu.VMEM((depth + 1,) + normal.shape, f32),
            pltpu.VMEM((depth,) + normal.shape, f32),
            pltpu.SemaphoreType.DMA((depth,)),
            pltpu.SemaphoreType.DMA((depth,)),
        ]
    if grad is not None:
        rows_t, grads = grad
        block = 2 * rows_t.shape[1] // count
        cols = grads.shape[1]
        args += [rows_t, grads]
        shapes.append(jax.ShapeDtypeStruct((block, cols), f32))
        grad_streams = cols // LANES
        scratch += [pltpu.VMEM((count, block, LANES), f32)] * grad_streams
        scratch += [pltpu.VMEM((count - 1, block, LANES), f32)] * grad_streams
    slots = 2 * state_streams + grad_streams
    scratch += [pltpu.SemaphoreType.DMA((slots, depth))] * 2
    out = pl.pallas_call(
        functools.partial(comm_kernel, count, state_streams, grad_streams),
        out_shape=tuple(shapes),
        in_specs=[pl.BlockSpec(memory_space=pltpu.VMEM)] * len(args),
        out_specs=tuple([pl.BlockSpec(memory_space=pltpu.VMEM)] * len(shapes)),
        scratch_shapes=scratch,
        compiler_params=pltpu.CompilerParams(
            collective_id=call, has_side_effects=True, vmem_limit_bytes=48 * 2**20
        ),
        name=f"exchange{call}",
    )(*args)
    out = list(out)
    if state is not None:
        out[0] = out[0].reshape(total.shape)
    return out


def features(rows, table, feat_count):
    logits = jnp.einsum("tgd,gdm->gtm", rows, table, precision=HIGHEST)
    half_norm = 0.5 * jnp.sum(rows * rows, axis=2).T
    return jnp.exp(logits - half_norm[:, :, None]) * feat_count ** (-0.5)


def feature_grad(rows, feats, grads, table, feature_scale, tok_count):
    weighted = feats * grads
    back = jnp.einsum("gtm,gdm->tgd", weighted, table, precision=HIGH)
    totals = jnp.sum(weighted, axis=2).T
    result = (back - rows * totals[:, :, None]) * feature_scale
    return result.reshape(tok_count, -1).astype(jnp.bfloat16)


def back_product(grads, weight):
    return lax.dot_general(
        grads, weight, (((1,), (1,)), ((), ())), preferred_element_type=jnp.float32
    )


def shards(count, hidden, query_weight, key_weight, values, grad_out, random_feats):
    tok_count, width = hidden.shape
    group_count, head_dim, feat_count = random_feats.shape
    feature_scale = head_dim ** (-0.25)
    rows_t = hidden.T.reshape(count // 2, 2, width // count, tok_count)
    rows_t = rows_t.transpose(1, 0, 2, 3).reshape(2, width // 2, tok_count)
    query_proj = jnp.dot(hidden, query_weight, preferred_element_type=jnp.float32)
    key_proj = jnp.dot(hidden, key_weight, preferred_element_type=jnp.float32)
    query_rows = (query_proj * feature_scale).reshape(tok_count, group_count, head_dim)
    key_rows = (key_proj * feature_scale).reshape(tok_count, group_count, head_dim)
    value_rows = values.astype(jnp.float32).reshape(tok_count, group_count, head_dim)
    key_feats = features(key_rows, random_feats, feat_count)
    local_state = jnp.einsum("tgj,gtm->gjm", value_rows, key_feats, precision=HIGH)
    local_normal = jnp.sum(key_feats, axis=1)
    value_state, normalizer = communicate(count, 0, state=(local_state, local_normal))
    query_feats = features(query_rows, random_feats, feat_count)
    numerator = jnp.einsum("gtm,gjm->tgj", query_feats, value_state, precision=HIGH)
    denominator = jnp.sum(query_feats * normalizer[:, None, :], axis=2).T
    attended = numerator / denominator[:, :, None]
    upstream = grad_out.astype(jnp.float32).reshape(tok_count, group_count, head_dim)
    grad_numer = upstream / denominator[:, :, None]
    grad_denom = -jnp.sum(upstream * attended, axis=2) / denominator
    grad_qfeat = (
        jnp.einsum("tgj,gjm->gtm", grad_numer, value_state, precision=HIGH)
        + grad_denom.T[:, :, None] * normalizer[:, None, :]
    )
    part_state = jnp.einsum("gtm,tgj->gjm", query_feats, grad_numer, precision=HIGH)
    part_normal = jnp.sum(query_feats * grad_denom.T[:, :, None], axis=1)
    grad_query = feature_grad(
        query_rows, query_feats, grad_qfeat, random_feats, feature_scale, tok_count
    )
    grad_state, grad_normal, grad_query_weight = communicate(
        count, 1, state=(part_state, part_normal), grad=(rows_t, grad_query)
    )
    grad_kfeat = (
        jnp.einsum("tgj,gjm->gtm", value_rows, grad_state, precision=HIGH) + grad_normal[:, None, :]
    )
    grad_value = jnp.einsum("gtm,gjm->tgj", key_feats, grad_state, precision=HIGH)
    grad_values = grad_value.reshape(tok_count, -1).astype(jnp.bfloat16)
    grad_key = feature_grad(key_rows, key_feats, grad_kfeat, random_feats, feature_scale, tok_count)
    (grad_key_weight,) = communicate(count, 2, grad=(rows_t, grad_key))
    both_parts = back_product(grad_query, query_weight) + back_product(grad_key, key_weight)
    grad_hidden = both_parts
    return (grad_hidden, grad_values, grad_query_weight, grad_key_weight)


def solution(mesh):
    placed = (
        P("seq", None),
        P(None, "head"),
        P(None, "head"),
        P("seq", "head"),
        P("seq", "head"),
        P("head", None, None),
    )

    def local(*args):
        out = shards(mesh.shape["seq"], *args)
        if mesh.shape["head"] == 1:
            return out
        return (lax.psum(out[0], "head"),) + tuple(out[1:])

    return jax.shard_map(
        local,
        mesh=mesh,
        in_specs=placed,
        out_specs=(P("seq", None), P("seq", "head"), P("seq", "head"), P("seq", "head")),
        check_vma=False,
    )
```

```python
import functools

import jax
import jax.numpy as jnp
from jax import lax
from jax.experimental import pallas as pl
from jax.experimental.pallas import tpu as pltpu
from jax.sharding import PartitionSpec as P

HIGHEST = lax.Precision.HIGHEST
HIGH = lax.Precision.HIGH
LANES = 128


def phase_orders(count):
    depth = count.bit_length() - 1
    middle = list(range(1, depth - 1))
    return [
        [(bit,) for bit in [0] + middle[s:] + middle[:s] + [depth - 1]] for s in range(3)
    ]


def wide_orders(count):
    depth = count.bit_length() - 1
    pairs = [tuple(range(b, min(b + 2, depth))) for b in range(1, depth, 2)]
    return [[(0,)] + pairs, [(0,)] + pairs[::-1]]


class Peers:
    def __init__(self, count):
        self.count = count
        self.depth = count.bit_length() - 1
        self.me = lax.axis_index("seq")
        self.bits = [(self.me // 2**b) % 2 for b in range(self.depth)]

    def reach(self, group):
        found = []
        for mask in range(1, 2 ** len(group)):
            index, digit, flips = self.me, 0, 0
            for j, b in enumerate(group):
                bit = self.bits[b]
                if (mask >> j) & 1:
                    index = index + (1 - 2 * bit) * 2**b
                    bit = 1 - bit
                    flips += 2**b
                digit = 2 * digit + bit
            found.append((flips, index, digit))
        return found

    def greet(self, orders):
        met = {}
        for order in orders:
            for group in order:
                for flips, index, _ in self.reach(group):
                    met[flips] = index
        barrier = pltpu.get_barrier_semaphore()
        for flips in sorted(met):
            pl.semaphore_signal(
                barrier, inc=1, device_id={"seq": met[flips]}, device_id_type=pl.DeviceIdType.MESH
            )
        pl.semaphore_wait(barrier, len(met))


def send(src, dst, sends, recvs, index):
    copy = pltpu.make_async_remote_copy(
        src_ref=src,
        dst_ref=dst,
        send_sem=sends,
        recv_sem=recvs,
        device_id={"seq": index},
        device_id_type=pl.DeviceIdType.MESH,
    )
    copy.start()
    return copy


class Halving:
    def __init__(self, peers, order, buf, recv, sends, recvs):
        self.peers, self.order = peers, order
        self.buf, self.recv, self.sends, self.recvs = buf, recv, sends, recvs
        self.offs, self.sizes = [0], [peers.count]
        for group in order:
            size = self.sizes[-1] // 2 ** len(group)
            digit = 0
            for b in group:
                digit = 2 * digit + peers.bits[b]
            self.offs.append(self.offs[-1] + digit * size)
            self.sizes.append(size)
        self.place = self.offs[-1]
        self.steps = len(order)

    def start(self, p):
        size = self.sizes[p + 1]
        base = self.peers.count - self.sizes[p]
        self.copies, self.landed = [], []
        for m, (_, index, digit) in enumerate(self.peers.reach(self.order[p])):
            slot = self.recv.at[pl.ds(base + m * size, size)]
            self.landed.append(slot)
            part = self.buf.at[pl.ds(self.offs[p] + digit * size, size)]
            self.copies.append(
                send(part, slot, self.sends.at[3 * p + m], self.recvs.at[3 * p + m], index)
            )

    def finish(self, p):
        kept = pl.ds(self.offs[p + 1], self.sizes[p + 1])
        for copy in self.copies:
            copy.wait()
        total = self.landed[0][...]
        for slot in self.landed[1:]:
            total = total + slot[...]
        self.buf[kept] += total


class Doubling:
    def __init__(self, halving, full, sends, recvs):
        self.halving, self.full, self.sends, self.recvs = halving, full, sends, recvs

    def load(self):
        place = pl.ds(self.halving.place, 1)
        self.full[place] = self.halving.buf[place]

    def start(self, p):
        h = self.halving
        owned = self.full.at[pl.ds(h.offs[p + 1], h.sizes[p + 1])]
        self.copies = [
            send(owned, owned, self.sends.at[3 * p + m], self.recvs.at[3 * p + m], index)
            for m, (_, index, _) in enumerate(h.peers.reach(h.order[p]))
        ]

    def finish(self, p):
        for copy in self.copies:
            copy.wait()


class SmallSum:
    def __init__(self, peers, order, sent, recv, sends, recvs):
        self.peers, self.order = peers, order
        self.sent, self.recv, self.sends, self.recvs = sent, recv, sends, recvs

    def start(self, p):
        self.copies = [
            send(
                self.sent.at[p],
                self.recv.at[3 * p + m],
                self.sends.at[3 * p + m],
                self.recvs.at[3 * p + m],
                index,
            )
            for m, (_, index, _) in enumerate(self.peers.reach(self.order[p]))
        ]

    def finish(self, p):
        for copy in self.copies:
            copy.wait()
        total = self.sent[p]
        for m in range(len(self.copies)):
            total = total + self.recv[3 * p + m]
        self.sent[p + 1] = total


def fill_blocks(halvings, side, rows_ref, grads_ref):
    count = halvings[0].peers.count
    block = halvings[0].buf.shape[1]
    rows = rows_ref.shape[1]
    step = min(rows, max(block, 256))
    for first in range(0, rows, step):
        part = jnp.dot(
            rows_ref[side, pl.ds(first, step), :], grads_ref[...], preferred_element_type=jnp.float32
        )
        for b in range(step // block):
            rest = first // block + b
            for s, h in enumerate(halvings):
                spot = sum(
                    ((rest >> (bit - 1)) & 1) * (count >> (p + 1))
                    for p, bit in enumerate(sum(h.order, ()))
                    if p > 0
                )
                h.buf[side * (count // 2) + spot] = part[
                    b * block : (b + 1) * block, s * LANES : (s + 1) * LANES
                ]


def comm_kernel(count, state_streams, grad_streams, *refs):
    refs = list(refs)
    take = lambda k: [refs.pop(0) for _ in range(k)]
    has_state, has_grad = state_streams > 0, grad_streams > 0
    if has_state:
        state_ref, normal_ref = take(2)
    if has_grad:
        rows_ref, grads_ref = take(2)
    if has_state:
        state_out, normal_out = take(2)
    if has_grad:
        (grad_out,) = take(1)
    if has_state:
        state_bufs, state_recvs, state_full = (take(state_streams) for _ in range(3))
        small_sent, small_recv, small_s, small_r = take(4)
    if has_grad:
        grad_bufs, grad_recvs = (take(grad_streams) for _ in range(2))
    sends, recvs = take(2)

    peers = Peers(count)
    orders, wide = phase_orders(count), wide_orders(count)
    depth, steps = peers.depth, len(wide[0])
    sums, small, outs, grads = [], [], [], []
    slot = 0
    if has_state:
        for s in range(state_streams):
            sums.append(
                Halving(peers, wide[s % 2], state_bufs[s], state_recvs[s], sends.at[slot], recvs.at[slot])
            )
            outs.append(Doubling(sums[-1], state_full[s], sends.at[slot + 1], recvs.at[slot + 1]))
            slot += 2
            state_bufs[s][...] = state_ref[:, :, s * LANES : (s + 1) * LANES]
        small.append(SmallSum(peers, wide[0], small_sent, small_recv, small_s, small_r))
        small_sent[0] = normal_ref[...]
    if has_grad:
        for s in range(grad_streams):
            order = orders[(s + state_streams) % 3]
            grads.append(Halving(peers, order, grad_bufs[s], grad_recvs[s], sends.at[slot], recvs.at[slot]))
            slot += 1

    peers.greet([h.order for h in sums + grads])
    for h in sums + small:
        h.start(0)
    if has_grad:
        core = peers.bits[0]
        fill_blocks(grads, 1 - core, rows_ref, grads_ref)
        for h in grads:
            h.start(0)
        fill_blocks(grads, core, rows_ref, grads_ref)

    def advance(step):
        for h in grads:
            if step < depth:
                h.finish(step)
            if step + 1 < depth:
                h.start(step + 1)

    done = 0
    if has_state:
        for p in range(steps):
            for h in sums + small:
                h.finish(p)
                if p + 1 < steps:
                    h.start(p + 1)
                elif h in sums:
                    gather = outs[sums.index(h)]
                    gather.load()
                    gather.start(steps - 1)
            if p > 0:
                advance(done)
                done += 1
        for p in reversed(range(steps)):
            for h in outs:
                h.finish(p)
                if p > 0:
                    h.start(p - 1)
            if p > 0:
                advance(done)
                done += 1
    for step in range(done, depth):
        advance(step)
    if has_state:
        for s in range(state_streams):
            state_out[:, :, s * LANES : (s + 1) * LANES] = state_full[s][...]
        normal_out[...] = small_sent[steps]
    for s, h in enumerate(grads):
        grad_out[:, s * LANES : (s + 1) * LANES] = h.buf[h.place]


def communicate(count, call, state=None, grad=None):
    depth = count.bit_length() - 1
    args, shapes, scratch = [], [], []
    f32 = jnp.float32
    state_streams = grad_streams = 0
    if state is not None:
        total, normal = state
        groups, head_dim, feats = total.shape
        rows = groups * head_dim // count
        args += [total.reshape(count, rows, feats), normal]
        shapes += [
            jax.ShapeDtypeStruct((count, rows, feats), f32),
            jax.ShapeDtypeStruct(normal.shape, f32),
        ]
        state_streams = feats // LANES
        scratch += [pltpu.VMEM((count, rows, LANES), f32)] * state_streams
        scratch += [pltpu.VMEM((count - 1, rows, LANES), f32)] * state_streams
        scratch += [pltpu.VMEM((count, rows, LANES), f32)] * state_streams
        scratch += [
            pltpu.VMEM((depth + 1,) + normal.shape, f32),
            pltpu.VMEM((3 * depth,) + normal.shape, f32),
            pltpu.SemaphoreType.DMA((3 * depth,)),
            pltpu.SemaphoreType.DMA((3 * depth,)),
        ]
    if grad is not None:
        rows_t, grads = grad
        block = 2 * rows_t.shape[1] // count
        cols = grads.shape[1]
        args += [rows_t, grads]
        shapes.append(jax.ShapeDtypeStruct((block, cols), f32))
        grad_streams = cols // LANES
        scratch += [pltpu.VMEM((count, block, LANES), f32)] * grad_streams
        scratch += [pltpu.VMEM((count - 1, block, LANES), f32)] * grad_streams
    slots = 2 * state_streams + grad_streams
    scratch += [pltpu.SemaphoreType.DMA((slots, 3 * depth))] * 2
    out = pl.pallas_call(
        functools.partial(comm_kernel, count, state_streams, grad_streams),
        out_shape=tuple(shapes),
        in_specs=[pl.BlockSpec(memory_space=pltpu.VMEM)] * len(args),
        out_specs=tuple([pl.BlockSpec(memory_space=pltpu.VMEM)] * len(shapes)),
        scratch_shapes=scratch,
        compiler_params=pltpu.CompilerParams(
            collective_id=call, has_side_effects=True, vmem_limit_bytes=48 * 2**20
        ),
        name=f"exchange{call}",
    )(*args)
    out = list(out)
    if state is not None:
        out[0] = out[0].reshape(total.shape)
    return out


def features(rows, table, feat_count):
    logits = jnp.einsum("tgd,gdm->gtm", rows, table, precision=HIGHEST)
    half_norm = 0.5 * jnp.sum(rows * rows, axis=2).T
    return jnp.exp(logits - half_norm[:, :, None]) * feat_count ** (-0.5)


def feature_grad(rows, feats, grads, table, feature_scale, tok_count):
    weighted = feats * grads
    back = jnp.einsum("gtm,gdm->tgd", weighted, table, precision=HIGH)
    totals = jnp.sum(weighted, axis=2).T
    result = (back - rows * totals[:, :, None]) * feature_scale
    return result.reshape(tok_count, -1).astype(jnp.bfloat16)


def back_product(grads, weight):
    return lax.dot_general(
        grads, weight, (((1,), (1,)), ((), ())), preferred_element_type=jnp.float32
    )


def shards(count, hidden, query_weight, key_weight, values, grad_out, random_feats):
    tok_count, width = hidden.shape
    group_count, head_dim, feat_count = random_feats.shape
    feature_scale = head_dim ** (-0.25)
    rows_t = hidden.T.reshape(count // 2, 2, width // count, tok_count)
    rows_t = rows_t.transpose(1, 0, 2, 3).reshape(2, width // 2, tok_count)
    query_proj = jnp.dot(hidden, query_weight, preferred_element_type=jnp.float32)
    key_proj = jnp.dot(hidden, key_weight, preferred_element_type=jnp.float32)
    query_rows = (query_proj * feature_scale).reshape(tok_count, group_count, head_dim)
    key_rows = (key_proj * feature_scale).reshape(tok_count, group_count, head_dim)
    value_rows = values.astype(jnp.float32).reshape(tok_count, group_count, head_dim)
    key_feats = features(key_rows, random_feats, feat_count)
    local_state = jnp.einsum("tgj,gtm->gjm", value_rows, key_feats, precision=HIGH)
    local_normal = jnp.sum(key_feats, axis=1)
    value_state, normalizer = communicate(count, 0, state=(local_state, local_normal))
    query_feats = features(query_rows, random_feats, feat_count)
    numerator = jnp.einsum("gtm,gjm->tgj", query_feats, value_state, precision=HIGH)
    denominator = jnp.sum(query_feats * normalizer[:, None, :], axis=2).T
    attended = numerator / denominator[:, :, None]
    upstream = grad_out.astype(jnp.float32).reshape(tok_count, group_count, head_dim)
    grad_numer = upstream / denominator[:, :, None]
    grad_denom = -jnp.sum(upstream * attended, axis=2) / denominator
    grad_qfeat = (
        jnp.einsum("tgj,gjm->gtm", grad_numer, value_state, precision=HIGH)
        + grad_denom.T[:, :, None] * normalizer[:, None, :]
    )
    part_state = jnp.einsum("gtm,tgj->gjm", query_feats, grad_numer, precision=HIGH)
    part_normal = jnp.sum(query_feats * grad_denom.T[:, :, None], axis=1)
    grad_query = feature_grad(
        query_rows, query_feats, grad_qfeat, random_feats, feature_scale, tok_count
    )
    grad_state, grad_normal, grad_query_weight = communicate(
        count, 1, state=(part_state, part_normal), grad=(rows_t, grad_query)
    )
    grad_kfeat = (
        jnp.einsum("tgj,gjm->gtm", value_rows, grad_state, precision=HIGH) + grad_normal[:, None, :]
    )
    grad_value = jnp.einsum("gtm,gjm->tgj", key_feats, grad_state, precision=HIGH)
    grad_values = grad_value.reshape(tok_count, -1).astype(jnp.bfloat16)
    grad_key = feature_grad(key_rows, key_feats, grad_kfeat, random_feats, feature_scale, tok_count)
    (grad_key_weight,) = communicate(count, 2, grad=(rows_t, grad_key))
    both_parts = back_product(grad_query, query_weight) + back_product(grad_key, key_weight)
    grad_hidden = both_parts
    return (grad_hidden, grad_values, grad_query_weight, grad_key_weight)


def solution(mesh):
    placed = (
        P("seq", None),
        P(None, "head"),
        P(None, "head"),
        P("seq", "head"),
        P("seq", "head"),
        P("head", None, None),
    )

    def local(*args):
        out = shards(mesh.shape["seq"], *args)
        if mesh.shape["head"] == 1:
            return out
        return (lax.psum(out[0], "head"),) + tuple(out[1:])

    return jax.shard_map(
        local,
        mesh=mesh,
        in_specs=placed,
        out_specs=(P("seq", None), P("seq", "head"), P("seq", "head"), P("seq", "head")),
        check_vma=False,
    )
```
